32 devices in a mesh: row: 4 (over z), col: 8 (over y, x, core).
Axes of the slice: x: 2, y: 2, z: 4, core: 2. Of those that a mesh axis runs over, the one named last changes fastest.
Arguments:
- tokens: bfloat16 [4096, 4096], P(('row', 'col')), may hold values from -6 to 6
- router_logits: float32 [4096, 32], P(('row', 'col')), may hold values from -15 to 320
- expert_ids: int32 [4096, 8], P(('row', 'col')), may hold values from 0 to 31, all different within a row; in each aligned block of 128 rows (0 to 127, 128 to 255, ...) at most 48 rows name the same one
- w_gate: bfloat16 [32, 4096, 768], P(('row', 'col')), may hold values from -0.09375 to 0.09375
- w_up: bfloat16 [32, 4096, 768], P(('row', 'col')), may hold values from -0.09375 to 0.09375
- w_down: bfloat16 [32, 768, 4096], P(('row', 'col')), may hold values from -0.21875 to 0.21875
Outputs:
- mixed: bfloat16 [4096, 4096], P(('row', 'col'))
- balance_loss: float32 [], replicated
The draws below stay inside these ranges and needn't reach their ends.
Inputs may be any that keep to these rules, and one draw needn't show every extreme that they name: `expert_ids`: each row names 8 different experts. In the 128 rows of one device no expert is named by more than 48 rows, a bound that some block reaches.
All inputs are finite; a program needn't handle non-finite values.
Results may differ from the reference program's by a relative error of at most 0.0015.
The reference program's roundings to bfloat16 on the way count: a program that leaves them out, or rounds other values in their place, can miss the bound.
Values may be sent and summed in bfloat16 or wider, within the bound.
A program may use at most 128 MiB of HBM per device.

```python
import math
import jax
import jax.numpy as jnp
import numpy as np
from jax import lax

D = 4096
FF = 768
TOPK = 8
TOK_DEV = 128
EXPERTS = 32
TOKENS = 4096
CAP = 48
N_ROW = 4
N_COL = 8


def draw_router_logits(key, part):
    base_key = jax.random.fold_in(key, 0)
    expert_key = jax.random.fold_in(key, 2)
    noise = 3.0 * jax.random.normal(base_key, (TOKENS, EXPERTS), jnp.float32)
    row_ids = jnp.arange(TOKENS)
    blocks = TOKENS // TOK_DEV
    block_of = (row_ids // TOK_DEV).astype(jnp.float32)
    rising = block_of / max(blocks - 1, 1)
    amplitude = 1.0 + 3.0 * rising
    expert_bias = 1.5 * jax.random.normal(expert_key, (EXPERTS,), jnp.float32)
    columns = jnp.arange(EXPERTS)
    phase = columns.astype(jnp.float32)[None, :] / EXPERTS - block_of[:, None] / blocks
    bias = amplitude[:, None] * jnp.cos(2.0 * jnp.pi * phase) + expert_bias[None, :]
    logits = jnp.clip(noise + bias, -15.0, 15.0)
    return logits


def levels(rng, dims, cuts, smallest, largest):
    def one(dim, shards_of):
        heights = jax.random.uniform(jax.random.fold_in(jax.random.fold_in(rng, 6), dim), (shards_of,), jnp.float32, smallest / len(cuts), largest / len(cuts))
        return jnp.repeat(jnp.exp(heights), dims[dim] // shards_of).reshape((-1,) + (1,) * (len(dims) - dim - 1))

    level = one(*cuts[0])
    for cut in cuts[1:]:
        level = level * one(*cut)
    return level


def assign_block(rng, own, number, rows, number_of, top, reach, lean):
    sequence = jax.random.permutation(rng, number_of)
    heavy_load, ordinary = load_shares(number_of, rows * top, reach, lean, True), load_shares(number_of, rows * top, reach, lean, False)
    places = jnp.arange(number_of)

    def named(tallies, offset_by):
        used = int((tallies > 0).sum())
        fixed = max(1, used // 4)
        shifted = fixed + (places - fixed + offset_by * (used - fixed)) % max(1, number_of - fixed)
        return jnp.zeros((number_of,), jnp.int32).at[sequence[jnp.where(places < fixed, places, shifted)]].set(jnp.asarray(tallies, jnp.int32))

    tallies = jnp.where(number % 4 == 0, named(heavy_load, number // 4), named(ordinary, number - number // 4 - 1))
    mixed = jax.random.permutation(jax.random.fold_in(own, 3), number_of)
    giver, taker = mixed[0:number_of // 2 * 2:2], mixed[1:number_of // 2 * 2:2]
    margin = jnp.minimum(tallies[giver] - 1, reach - tallies[taker]) // 2
    margin = jnp.where((giver == sequence[0]) | (taker == sequence[0]) | (tallies[taker] == 0), 0, jnp.maximum(margin, 0))
    shifted = jax.random.randint(jax.random.fold_in(own, 4), (number_of // 2,), 0, 1 << 20) % (margin + 1)
    tallies = tallies.at[giver].add(-shifted).at[taker].add(shifted)
    members = jnp.searchsorted(jnp.cumsum(tallies), jnp.arange(rows * top), side="right").astype(jnp.int32)
    table = members.reshape(top, rows).T
    table = table[jax.random.permutation(jax.random.fold_in(own, 1), rows)]
    offset_by = jax.random.randint(jax.random.fold_in(own, 2), (rows, 1), 0, top)
    return jnp.take_along_axis(table, (jnp.arange(top)[None, :] + offset_by) % top, axis=1)


def load_shares(number_of, total, most, lean, full):
    loads = [(1 << 20) // math.isqrt(grade ** lean) + 1 for grade in range(1, number_of + 1)]
    largest = most if full else min(most, max(-(-total // number_of), total * loads[0] // sum(loads)))
    least = 1 if total - largest >= number_of - 1 else 0
    holding, surplus = [largest] + [least] * (number_of - 1), total - largest - least * (number_of - 1)
    while surplus > 0:
        free = [i for i in range(1, number_of) if holding[i] < largest] or [i for i in range(1, number_of) if holding[i] < most]
        whole, budget = sum([loads[i] for i in free]), surplus
        for i in free:
            extra = min(most - holding[i], max(1, budget * loads[i] // whole), surplus)
            holding[i] = holding[i] + extra
            surplus = surplus - extra
    return np.array(holding)


def normal_values(key, extent, width, most, shards=(), held_as=jnp.bfloat16):
    gain = levels(key, extent, shards, -0.22, 0.18) if shards else 1.0
    drawn = jax.random.normal(key, extent, jnp.float32) * width * gain
    return jnp.minimum(jnp.maximum(drawn, -most), most).astype(held_as)


def setup_inputs(seed: int = 0) -> dict:
    arg_keys = jax.random.split(jax.random.key(seed), 7)
    tokens = normal_values(arg_keys[0], (TOKENS, D), 1.0, 6.0, ((0, 32),))
    router_logits = draw_router_logits(jax.random.fold_in(arg_keys[6], 71), 0)
    expert_ids_keys = jax.random.split(jax.random.fold_in(arg_keys[2], 1), TOKENS // TOK_DEV)
    expert_ids_turns = jax.random.permutation(jax.random.fold_in(arg_keys[2], 3), TOKENS // TOK_DEV)
    expert_ids = jax.vmap(lambda own, number: assign_block(jax.random.fold_in(arg_keys[2], 2), own, number, TOK_DEV, EXPERTS, TOPK, CAP, 2))(expert_ids_keys, expert_ids_turns).reshape((TOKENS, TOPK))
    w_gate = normal_values(arg_keys[3], (EXPERTS, D, FF), D ** -0.5, 0.09375, ((0, 32),))
    w_up = normal_values(arg_keys[4], (EXPERTS, D, FF), D ** -0.5, 0.09375, ((0, 32),))
    w_down = normal_values(arg_keys[5], (EXPERTS, FF, D), FF ** -0.5, 0.21875, ((0, 32),))
    return {"tokens": tokens, "router_logits": router_logits, "expert_ids": expert_ids, "w_gate": w_gate, "w_up": w_up, "w_down": w_down}


def slot_table(expert_ids, experts, capacity):
    flattened = expert_ids.reshape(-1)
    onehot = (flattened[:, None] == jnp.arange(experts, dtype=jnp.int32)[None, :]).astype(jnp.int32)
    earlier = jnp.cumsum(onehot, axis=0) - onehot
    slot_of = jnp.sum(earlier * onehot, axis=1)
    position = flattened * capacity + slot_of
    return onehot, position.astype(jnp.int32)


def reference(tokens, router_logits, expert_ids, w_gate, w_up, w_down):
    blocks = N_ROW * N_COL
    assigned = TOK_DEV * TOPK
    probs = jax.nn.softmax(router_logits.astype(jnp.float32), axis=1)
    chosen = jnp.take_along_axis(probs, expert_ids, axis=1)
    weights = chosen / jnp.sum(chosen, axis=1, keepdims=True)
    grouped_ids = expert_ids.reshape(blocks, TOK_DEV, TOPK)
    onehot, position = jax.vmap(slot_table, in_axes=(0, None, None))(grouped_ids, EXPERTS, CAP)
    block_ids = jnp.arange(blocks, dtype=jnp.int32)
    source = block_ids[:, None] * TOK_DEV + jnp.arange(assigned, dtype=jnp.int32)[None, :] // TOPK
    owner = jnp.full((blocks, EXPERTS * CAP), -1, jnp.int32).at[block_ids[:, None], position].set(source)
    weight_table = jnp.zeros((blocks, EXPERTS * CAP), jnp.float32).at[block_ids[:, None], position].set(weights.reshape(blocks, assigned))
    owner = owner.reshape(blocks, EXPERTS, CAP).transpose(1, 0, 2).reshape(EXPERTS, blocks * CAP)
    weight_table = weight_table.reshape(blocks, EXPERTS, CAP).transpose(1, 0, 2).reshape(EXPERTS, blocks * CAP)

    def one_expert(total, inputs):
        owner_e, weight_e, gate_e, up_e, down_e = inputs
        present = owner_e >= 0
        safe = jnp.maximum(owner_e, 0).astype(jnp.int32)
        slot_rows = jnp.where(present[:, None], tokens[safe], jnp.zeros((), jnp.bfloat16))
        gate_act = jnp.dot(slot_rows, gate_e, preferred_element_type=jnp.float32)
        up_act = jnp.dot(slot_rows, up_e, preferred_element_type=jnp.float32)
        hidden = (jax.nn.silu(gate_act) * up_act).astype(jnp.bfloat16)
        result = jnp.dot(hidden, down_e, preferred_element_type=jnp.float32).astype(jnp.bfloat16)
        total = total.at[safe].add(weight_e[:, None] * result.astype(jnp.float32))
        return total, None

    start = jnp.zeros((TOKENS, D), jnp.float32)
    total, unused = lax.scan(one_expert, start, (owner, weight_table, w_gate, w_up, w_down))
    mixed = total.astype(jnp.bfloat16)
    counts = jnp.sum(onehot, axis=(0, 1)).astype(jnp.float32)
    prob_total = jnp.sum(probs, axis=0)
    balance_loss = EXPERTS * jnp.sum((counts / (TOKENS * TOPK)) * (prob_total / TOKENS))
    return mixed, balance_loss
```

```python
import jax
import jax.numpy as jnp
from jax import lax
from jax.sharding import PartitionSpec as P

BF16 = jnp.bfloat16
F32 = jnp.float32
AXES = ("row", "col")
CHUNKS = 4
GATHER_LIMIT = 64 * 1024 * 1024


def slots_before(hit):
    tok = hit.shape[-1]
    order = jnp.arange(tok, dtype=jnp.int32)
    upper = (order[:, None] < order[None, :]).astype(BF16)
    return jnp.dot(hit.astype(BF16), upper, preferred_element_type=F32)


def exchange_routes(router_logits, expert_ids):
    tok, top_k = expert_ids.shape
    experts = router_logits.shape[1]
    probs = jax.nn.softmax(router_logits, axis=1)
    names = jnp.arange(experts, dtype=jnp.int32)
    match = expert_ids[:, :, None] == names[None, None, :]
    chosen = jnp.sum(jnp.where(match, probs[:, None, :], 0.0), axis=2)
    weights = chosen / jnp.sum(chosen, axis=1, keepdims=True)
    prob_rows = -(-experts // tok)
    prob_sum = jnp.pad(jnp.sum(probs, axis=0), (0, prob_rows * tok - experts)).reshape(prob_rows, tok)
    packed = jnp.concatenate([expert_ids.astype(F32).T, weights.T, prob_sum], axis=0)
    routes = lax.all_gather(packed, AXES, axis=0, tiled=False)
    ids = routes[:, :top_k].astype(jnp.int32)
    mix = routes[:, top_k : 2 * top_k]
    prob_total = jnp.sum(routes[:, 2 * top_k :], axis=0).reshape(-1)[:experts]
    return ids, mix, prob_total


def local(tokens, router_logits, expert_ids, w_gate, w_up, w_down):
    tok, top_k = expert_ids.shape
    width = tokens.shape[1]
    experts = router_logits.shape[1]
    n_row = lax.axis_size("row")
    n_col = lax.axis_size("col")
    n_dev = n_row * n_col
    capacity = 3 * tok * top_k // (2 * experts)
    row, col = lax.axis_index("row"), lax.axis_index("col")
    me = row * n_col + col

    ids, mix, prob_total = exchange_routes(router_logits, expert_ids)
    names = jnp.arange(experts, dtype=jnp.int32)
    counts = jnp.sum((ids[..., None] == names).astype(F32), axis=(0, 1, 2))
    tokens_all = tok * n_dev
    balance_loss = experts * jnp.sum(counts / (tokens_all * top_k) * (prob_total / tokens_all))
    places = jnp.arange(capacity, dtype=F32)

    if tokens.size * tokens.dtype.itemsize * n_dev <= GATHER_LIMIT:
        hit = jnp.any(ids == me, axis=1)
        slot = slots_before(hit)
        pick = (hit[:, None, :] & (slot[:, None, :] == places[None, :, None])).astype(BF16)
        everyone = lax.all_gather(tokens, AXES, axis=0, tiled=False)
        rows = lax.dot_general(
            pick, everyone, (((2,), (1,)), ((0,), (0,))), preferred_element_type=F32
        ).astype(BF16)
    else:
        mine = lax.dynamic_index_in_dim(ids, me, 0, keepdims=False)
        hit = jnp.any(mine[None] == names[:, None, None], axis=1)
        slot = slots_before(hit)
        pick = (hit[:, None, :] & (slot[:, None, :] == places[None, :, None])).astype(BF16)
        picked = lax.dot_general(
            pick.reshape(-1, tok), tokens, (((1,), (0,)), ((), ())), preferred_element_type=F32
        ).astype(BF16)
        rows = lax.all_to_all(
            picked.reshape(experts, capacity, width), AXES, split_axis=0, concat_axis=0, tiled=True
        )
    shaped = rows.reshape(n_dev * capacity, width)
    gate_act = jnp.dot(shaped, w_gate[0], preferred_element_type=F32)
    up_act = jnp.dot(shaped, w_up[0], preferred_element_type=F32)
    hidden = (jax.nn.silu(gate_act) * up_act).astype(BF16)
    hidden = hidden.reshape(n_row, n_col, capacity, -1).swapaxes(0, 1).reshape(n_dev * capacity, -1)

    column_ids = lax.dynamic_index_in_dim(ids.reshape(n_row, n_col, top_k, tok), col, 1, keepdims=False)
    column_mix = lax.dynamic_index_in_dim(mix.reshape(n_row, n_col, top_k, tok), col, 1, keepdims=False)
    row_names = row * n_col + jnp.arange(n_col, dtype=jnp.int32)
    match = column_ids[:, None] == row_names[None, :, None, None]
    hit = jnp.any(match, axis=2)
    share = jnp.sum(jnp.where(match, column_mix[:, None], 0.0), axis=2)
    slot = slots_before(hit)
    here = slot[:, :, None, :] == places[None, None, :, None]
    high = lax.reduce_precision(share, 8, 7)
    low = lax.reduce_precision(share - high, 8, 7)

    def table(part):
        return jnp.where(here, part[:, :, None, :], 0.0).astype(BF16).reshape(n_row, n_col * capacity, tok)

    high, low = table(high), table(low)

    step = width // CHUNKS
    parts = []
    for chunk in range(CHUNKS):
        down = w_down[0][:, chunk * step : (chunk + 1) * step]
        result = jnp.dot(hidden, down, preferred_element_type=F32).astype(BF16)
        back = lax.all_to_all(
            result.reshape(n_col, n_row, capacity, step), "col", split_axis=0, concat_axis=0, tiled=True
        )
        back = back.swapaxes(0, 1).reshape(n_row, n_col * capacity, step)
        dims = (((1,), (1,)), ((0,), (0,)))
        partial = lax.dot_general(high, back, dims, preferred_element_type=F32)
        partial = partial + lax.dot_general(low, back, dims, preferred_element_type=F32)
        total = lax.psum_scatter(partial, "row", scatter_dimension=0, tiled=True)
        parts.append(total.reshape(tok, step).astype(BF16))
    return jnp.concatenate(parts, axis=1), balance_loss


def solution(mesh):
    placed = (
        P(AXES, None),
        P(AXES, None),
        P(AXES, None),
        P(AXES, None, None),
        P(AXES, None, None),
        P(AXES, None, None),
    )
    return jax.shard_map(
        local, mesh=mesh, in_specs=placed, out_specs=(P(AXES, None), P()), check_vma=False
    )
```

```python
import jax
import jax.numpy as jnp
from jax import lax
from jax.experimental import pallas as pl
from jax.experimental.pallas import tpu as pltpu
from jax.sharding import PartitionSpec as P

BF16 = jnp.bfloat16
F32 = jnp.float32
AXES = ("row", "col")
CHUNK_EIGHTHS = (1, 2, 2, 2, 1)
ROUTES_MIN = 1024 * 1024
GATHER_LIMIT = 64 * 1024 * 1024


def slots_before(hit):
    tok = hit.shape[-1]
    order = jnp.arange(tok, dtype=jnp.int32)
    upper = (order[:, None] < order[None, :]).astype(BF16)
    return jnp.dot(hit.astype(BF16), upper, preferred_element_type=F32)


def exchange_routes(router_logits, expert_ids):
    tok, top_k = expert_ids.shape
    experts = router_logits.shape[1]
    probs = jax.nn.softmax(router_logits, axis=1)
    names = jnp.arange(experts, dtype=jnp.int32)
    match = expert_ids[:, :, None] == names[None, None, :]
    chosen = jnp.sum(jnp.where(match, probs[:, None, :], 0.0), axis=2)
    weights = chosen / jnp.sum(chosen, axis=1, keepdims=True)
    prob_rows = -(-experts // tok)
    prob_sum = jnp.pad(jnp.sum(probs, axis=0), (0, prob_rows * tok - experts)).reshape(prob_rows, tok)
    packed = jnp.concatenate([expert_ids.astype(F32).T, weights.T, prob_sum], axis=0)
    whole = lax.axis_size("row") * lax.axis_size("col") * tok * packed.dtype.itemsize
    packed = jnp.pad(packed, ((0, max(0, -(-ROUTES_MIN // whole) - packed.shape[0])), (0, 0)))
    routes = lax.all_gather(packed, AXES, axis=0, tiled=False)
    ids = routes[:, :top_k].astype(jnp.int32)
    mix = routes[:, top_k : 2 * top_k]
    prob_total = jnp.sum(routes[:, 2 * top_k : 2 * top_k + prob_rows], axis=0).reshape(-1)[:experts]
    return ids, mix, prob_total


def flip(index, bit):
    return index + bit - 2 * bit * ((index // bit) % 2)


def gather_kernel(n_row, tok_ref, out_ref, own_sem, send_sems, recv_sems):
    row, col = lax.axis_index("row"), lax.axis_index("col")
    col_c, col_x, col_y = flip(col, 1), flip(col, 2), flip(col, 4)
    col_d = flip(col_x, 4)

    def peer_row(k):
        there = row
        bit = 1
        while bit < n_row:
            if k & bit:
                there = flip(there, bit)
            bit *= 2
        return there

    rows = [peer_row(k) for k in range(n_row)]

    barrier = pltpu.get_barrier_semaphore()
    peers = [(rows[k], col) for k in range(1, n_row)] + [(row, c) for c in (col_c, col_x, col_y)]
    for peer in peers:
        pl.semaphore_signal(barrier, inc=1, device_id=peer, device_id_type=pl.DeviceIdType.MESH)
    pl.semaphore_wait(barrier, len(peers))

    def copy(k, kind, src, dst, device):
        return pltpu.make_async_remote_copy(
            src_ref=src,
            dst_ref=dst,
            send_sem=send_sems.at[k, kind],
            recv_sem=recv_sems.at[k, kind],
            device_id=device,
            device_id_type=pl.DeviceIdType.MESH,
        )

    started = []

    def send(*args):
        one = copy(*args)
        one.start()
        started.append(one)

    def arrived(k, kind, ref):
        copy(k, kind, ref, ref, (row, col_c)).wait_recv()

    def spread(k):
        origin = out_ref.at[rows[k], col]
        source = tok_ref if k == 0 else origin
        for half in range(2):
            send(k, 1 + half, source.at[half], origin.at[half], (row, col_x))
            send(k, 3 + half, source.at[half], origin.at[half], (row, col_y))
        send(k, 7, source, origin, (row, col_c))

    own = pltpu.make_async_copy(tok_ref, out_ref.at[row, col], own_sem)
    for k in range(1, n_row):
        send(k, 0, tok_ref, out_ref.at[row, col], (rows[k], col))
    spread(0)
    own.start()
    for k in range(n_row):
        if k + 1 < n_row:
            arrived(k + 1, 0, out_ref.at[rows[k + 1], col])
            spread(k + 1)
        from_x, from_y = out_ref.at[rows[k], col_x], out_ref.at[rows[k], col_y]
        arrived(k, 3, from_y.at[0])
        send(k, 5, from_y.at[0], from_y.at[0], (row, col_x))
        arrived(k, 2, from_x.at[1])
        send(k, 6, from_x.at[1], from_x.at[1], (row, col_y))
        arrived(k, 1, from_x.at[0])
        send(k, 8, from_x, from_x, (row, col_c))
        arrived(k, 4, from_y.at[1])
        send(k, 9, from_y, from_y, (row, col_c))
    for k in range(n_row):
        diagonal = out_ref.at[rows[k], col_d]
        arrived(k, 5, diagonal.at[0])
        arrived(k, 6, diagonal.at[1])
        send(k, 10, diagonal, diagonal, (row, col_c))
    for k in range(n_row):
        for kind, place in ((7, col), (8, col_x), (9, col_y), (10, col_d)):
            arrived(k, kind, out_ref.at[rows[k], flip(place, 1)])
    own.wait()
    for one in started:
        one.wait_send()


def gather_tokens(tokens, n_row, n_col):
    tok, width = tokens.shape
    if n_col != 8 or n_row & (n_row - 1):
        return lax.all_gather(tokens, AXES, axis=0, tiled=False)
    kinds = 11
    out = pl.pallas_call(
        lambda *refs: gather_kernel(n_row, *refs),
        out_shape=jax.ShapeDtypeStruct((n_row, n_col, 2, tok // 2, width), tokens.dtype),
        in_specs=[pl.BlockSpec(memory_space=pltpu.VMEM)],
        out_specs=pl.BlockSpec(memory_space=pl.ANY),
        scratch_shapes=[
            pltpu.SemaphoreType.DMA(()),
            pltpu.SemaphoreType.DMA((n_row, kinds)),
            pltpu.SemaphoreType.DMA((n_row, kinds)),
        ],
        compiler_params=pltpu.CompilerParams(collective_id=0, has_side_effects=True),
        cost_estimate=pl.CostEstimate(flops=0, bytes_accessed=300 * 1024 * 1024, transcendentals=0),
    )(tokens.reshape(2, tok // 2, width))
    return out.reshape(n_row * n_col, tok, width)


def local(tokens, router_logits, expert_ids, w_gate, w_up, w_down):
    tok, top_k = expert_ids.shape
    width = tokens.shape[1]
    experts = router_logits.shape[1]
    n_row = lax.axis_size("row")
    n_col = lax.axis_size("col")
    n_dev = n_row * n_col
    capacity = 3 * tok * top_k // (2 * experts)
    row, col = lax.axis_index("row"), lax.axis_index("col")
    me = row * n_col + col

    ids, mix, prob_total = exchange_routes(router_logits, expert_ids)
    names = jnp.arange(experts, dtype=jnp.int32)
    counts = jnp.sum((ids[..., None] == names).astype(F32), axis=(0, 1, 2))
    tokens_all = tok * n_dev
    balance_loss = experts * jnp.sum(counts / (tokens_all * top_k) * (prob_total / tokens_all))
    places = jnp.arange(capacity, dtype=F32)

    if tokens.size * tokens.dtype.itemsize * n_dev <= GATHER_LIMIT:
        hit = jnp.any(ids == me, axis=1)
        slot = slots_before(hit)
        pick = (hit[:, None, :] & (slot[:, None, :] == places[None, :, None])).astype(BF16)
        everyone = gather_tokens(tokens, n_row, n_col)
        rows = lax.dot_general(
            pick, everyone, (((2,), (1,)), ((0,), (0,))), preferred_element_type=F32
        ).astype(BF16)
    else:
        mine = lax.dynamic_index_in_dim(ids, me, 0, keepdims=False)
        hit = jnp.any(mine[None] == names[:, None, None], axis=1)
        slot = slots_before(hit)
        pick = (hit[:, None, :] & (slot[:, None, :] == places[None, :, None])).astype(BF16)
        picked = lax.dot_general(
            pick.reshape(-1, tok), tokens, (((1,), (0,)), ((), ())), preferred_element_type=F32
        ).astype(BF16)
        rows = lax.all_to_all(
            picked.reshape(experts, capacity, width), AXES, split_axis=0, concat_axis=0, tiled=True
        )
    shaped = rows.reshape(n_dev * capacity, width)
    gate_act = jnp.dot(shaped, w_gate[0], preferred_element_type=F32)
    up_act = jnp.dot(shaped, w_up[0], preferred_element_type=F32)
    hidden = (jax.nn.silu(gate_act) * up_act).astype(BF16)
    hidden = hidden.reshape(n_row, n_col, capacity, -1).swapaxes(0, 1).reshape(n_dev * capacity, -1)

    column_ids = lax.dynamic_index_in_dim(ids.reshape(n_row, n_col, top_k, tok), col, 1, keepdims=False)
    column_mix = lax.dynamic_index_in_dim(mix.reshape(n_row, n_col, top_k, tok), col, 1, keepdims=False)
    row_names = row * n_col + jnp.arange(n_col, dtype=jnp.int32)
    match = column_ids[:, None] == row_names[None, :, None, None]
    hit = jnp.any(match, axis=2)
    share = jnp.sum(jnp.where(match, column_mix[:, None], 0.0), axis=2)
    slot = slots_before(hit)
    here = slot[:, :, None, :] == places[None, None, :, None]
    high = lax.reduce_precision(share, 8, 7)
    low = lax.reduce_precision(share - high, 8, 7)

    def table(part):
        return jnp.where(here, part[:, :, None, :], 0.0).astype(BF16).reshape(n_row, n_col * capacity, tok)

    high, low = table(high), table(low)

    parts = []
    start = 0
    for eighths in CHUNK_EIGHTHS:
        step = eighths * width // 8
        down = w_down[0][:, start : start + step]
        start += step
        result = jnp.dot(hidden, down, preferred_element_type=F32).astype(BF16)
        back = lax.all_to_all(
            result.reshape(n_col, n_row, capacity, step), "col", split_axis=0, concat_axis=0, tiled=True
        )
        back = back.swapaxes(0, 1).reshape(n_row, n_col * capacity, step)
        dims = (((1,), (1,)), ((0,), (0,)))
        partial = lax.dot_general(high, back, dims, preferred_element_type=F32)
        partial = partial + lax.dot_general(low, back, dims, preferred_element_type=F32)
        total = lax.psum_scatter(partial, "row", scatter_dimension=0, tiled=True)
        parts.append(total.reshape(tok, step).astype(BF16))
    return jnp.concatenate(parts, axis=1), balance_loss


def solution(mesh):
    placed = (
        P(AXES, None),
        P(AXES, None),
        P(AXES, None),
        P(AXES, None, None),
        P(AXES, None, None),
        P(AXES, None, None),
    )
    return jax.shard_map(
        local, mesh=mesh, in_specs=placed, out_specs=(P(AXES, None), P()), check_vma=False
    )
```
